512 devices in a mesh: req: 64 (over y, x, z_lo), tp: 8 (over z_hi, core).
Axes of the slice: x: 4, y: 8, z: 8 (z_hi: 4, z_lo: 2; z = z_hi * 2 + z_lo), core: 2. Of those that a mesh axis runs over, the one named last changes fastest.
Arguments:
- tree_queries: bfloat16 [64, 512, 4096], P('req', None, 'tp'), may hold values from -512 to 512
- tree_keys: bfloat16 [64, 512, 512], P('req', None, 'tp'), may hold values from -6 to 6
- tree_values: bfloat16 [64, 512, 512], P('req', None, 'tp'), may hold values from -6 to 6
- cache_keys: bfloat16 [64, 1024, 512], P('req', None, 'tp'), may hold values from -6 to 6
- cache_values: bfloat16 [64, 1024, 512], P('req', None, 'tp'), may hold values from -6 to 6
- sinks: float32 [64], P('tp'), may hold values from 7 to 11
- parents: int32 [64, 512], P('req'), may hold values from 0 to 510, as said below
- tile_counts: int32 [64], P('req'), may hold values from 1 to 4, 128 in all
- out_weight: bfloat16 [4096, 2880], P('tp', 'req'), may hold values from -0.71875 to 0.71875
Outputs:
- mixed: bfloat16 [64, 512, 2880], P('req', 'tp')
The draws below stay inside these ranges and needn't reach their ends.
Inputs may be any that keep to these rules, and one draw needn't show every extreme that they name: `parents`: each position's parent stands before it; position 0 is its own parent. `tile_counts`: the counts sum to 128.
All inputs are finite; a program needn't handle non-finite values. No bound on the sum of `tile_counts` on one device may be relied on, other than what follows from the above.
Results may differ from the reference program's by a relative error of at most 0.024.
Values may be sent and summed in bfloat16 or wider, within the bound.
A program may use at most 64 MiB of HBM per device.

```python
import math
import jax
import jax.numpy as jnp
import numpy as np
from jax import lax

D = 2880
HEADS = 64
KV_HEADS = 8
HEAD_DIM = 64
TREE = 512
TILE = 128
CTX = 1024
REQS = 64
N_TP = 8


def shared_keys(key):
    array_shape = (REQS, CTX, KV_HEADS * HEAD_DIM)
    drawn = jnp.clip(jax.random.normal(jax.random.fold_in(key, 7), array_shape, jnp.float32), -6.0, 6.0)
    return drawn


def draw_cache_keys(key, part):
    return shared_keys(key).astype(jnp.bfloat16)


def draw_tree_queries(key, part):
    array_shape = (REQS, TREE, HEADS * HEAD_DIM)
    drawn = 2.0 * jnp.clip(jax.random.normal(jax.random.fold_in(key, 3), array_shape, jnp.float32), -6.0, 6.0)
    return drawn.astype(jnp.bfloat16)


def draw_parents(key, part):
    positions = jnp.arange(TREE, dtype=jnp.int32)
    chooser = jax.random.randint(jax.random.fold_in(key, 1), (REQS, TREE), 0, 10)
    anywhere = jax.random.randint(jax.random.fold_in(key, 2), (REQS, TREE), 0, TREE) % jnp.maximum(positions, 1)
    parent_row = jnp.where(chooser < 7, positions - 1, anywhere)
    return jnp.maximum(parent_row, 0).astype(jnp.int32)


def block_scale(key, dims, cuts, low, high):
    def one(dim, shards_of):
        draws = jax.random.uniform(jax.random.fold_in(jax.random.fold_in(key, 6), dim), (shards_of,), jnp.float32, low / len(cuts), high / len(cuts))
        return jnp.repeat(jnp.exp(draws), dims[dim] // shards_of).reshape((-1,) + (1,) * (len(dims) - dim - 1))

    gain = one(*cuts[0])
    for cut in cuts[1:]:
        gain = gain * one(*cut)
    return gain


def profile(amount, total, bound, slope):
    loads = [(1 << 20) // math.isqrt(grade ** slope) + 1 for grade in range(2, amount + 1)]
    rest, holding = total - bound - (amount - 1), [1] * (amount - 1)
    while rest > 0:
        candidates = [i for i in range(amount - 1) if holding[i] < bound]
        whole, remaining = sum([loads[i] for i in candidates]), rest
        for i in candidates:
            extra = min(bound - holding[i], max(1, remaining * loads[i] // whole), rest)
            holding[i] = holding[i] + extra
            rest = rest - extra
    return np.array([bound] + holding)


def ragged(key, count, total, reach, slope):
    if count == 2:
        one = jax.random.randint(key, (), max(1, total - reach), min(reach, total - 1) + 1)
        return jnp.stack([one, total - one])
    tallies = jnp.asarray(profile(count, total, reach, slope), jnp.int32)
    twos = (count - 1) // 2
    donor, sink = tallies[1:1 + 2 * twos:2], tallies[2:2 + 2 * twos:2]
    room = jnp.minimum(donor - 1, reach - sink)
    passed = jax.random.randint(jax.random.fold_in(key, 1), (twos,), 0, 1 << 20) % (room + 1)
    tallies = tallies.at[1:1 + 2 * twos:2].set(donor - passed).at[2:2 + 2 * twos:2].set(sink + passed)
    return tallies[jax.random.permutation(jax.random.fold_in(key, 2), count)]


def gaussian(own_key, extent, spread, bound, split=(), held_as=jnp.bfloat16):
    result = spread * jax.random.normal(own_key, extent, jnp.float32)
    if split:
        result = result * block_scale(own_key, extent, split, -0.22, 0.18)
    return jnp.clip(result, -bound, bound).astype(held_as)


def setup_inputs(seed: int = 0) -> dict:
    splits = jax.random.split(jax.random.key(seed), 10)
    return {
        "tree_queries": draw_tree_queries(jax.random.fold_in(splits[9], 71), 0),
        "tree_keys": gaussian(splits[1], (REQS, TREE, KV_HEADS * HEAD_DIM), 1.0, 6.0, ((0, 64), (2, 8))),
        "tree_values": gaussian(splits[2], (REQS, TREE, KV_HEADS * HEAD_DIM), 1.0, 6.0, ((0, 64), (2, 8))),
        "cache_keys": draw_cache_keys(jax.random.fold_in(splits[9], 71), 0),
        "cache_values": gaussian(splits[4], (REQS, CTX, KV_HEADS * HEAD_DIM), 1.0, 6.0, ((0, 64), (2, 8))),
        "sinks": jnp.clip(7.0 + 4.0 * jax.random.uniform(splits[5], (HEADS,), jnp.float32) ** block_scale(splits[5], (HEADS,), ((0, 8),), -0.2, 0.2), 7.0, 11.0),
        "parents": draw_parents(jax.random.fold_in(splits[9], 71), 0),
        "tile_counts": ragged(splits[7], REQS, 2 * REQS, TREE // TILE, 2).astype(jnp.int32),
        "out_weight": gaussian(splits[8], (HEADS * HEAD_DIM, D), 0.12, 0.71875, ((0, 8), (1, 64))),
    }


masked_score = -1e30


def ancestry(parents):
    length = parents.shape[0]
    upward = parents
    visible = jnp.eye(length, dtype=jnp.int32)
    doubling = 0
    while (1 << doubling) < length:
        visible = jnp.maximum(visible, jnp.take(visible, upward, axis=0))
        upward = jnp.take(upward, upward, axis=0)
        doubling += 1
    return visible


def request_attention(queries, tree_keys, tree_values, cache_keys, cache_values, sinks, parents, live_tiles):
    group_size = HEADS // KV_HEADS
    visible = ancestry(parents)
    scaling = HEAD_DIM ** -0.5
    query_heads = queries.astype(jnp.float32).reshape(TREE, KV_HEADS, group_size, HEAD_DIM).transpose(1, 0, 2, 3)
    all_keys = jnp.concatenate([cache_keys, tree_keys], 0).astype(jnp.float32).reshape(CTX + TREE, KV_HEADS, HEAD_DIM).transpose(1, 0, 2)
    all_values = jnp.concatenate([cache_values, tree_values], 0).astype(jnp.float32).reshape(CTX + TREE, KV_HEADS, HEAD_DIM).transpose(1, 0, 2)
    allowed = jnp.concatenate([jnp.ones((TREE, CTX), dtype=jnp.int32), visible], 1) > 0
    sink_heads = sinks.reshape(KV_HEADS, group_size)

    def per_head(operands):
        query_block, key_block, value_block, sink_row = operands
        scores = jnp.einsum("tgd,cd->gtc", query_block, key_block) * scaling
        scores = jnp.where(allowed[None], scores, masked_score)
        maxima = jnp.maximum(scores.max(-1), sink_row[:, None])
        weights = jnp.exp(scores - maxima[..., None])
        denominator = weights.sum(-1) + jnp.exp(sink_row[:, None] - maxima)
        rounded = weights.astype(jnp.bfloat16).astype(jnp.float32)
        weighted = jnp.einsum("gtc,cd->gtd", rounded, value_block)
        return weighted / denominator[..., None]

    per_heads = lax.map(per_head, (query_heads, all_keys, all_values, sink_heads))
    attention = per_heads.transpose(2, 0, 1, 3).reshape(TREE, HEADS * HEAD_DIM)
    live_rows = jnp.arange(TREE, dtype=jnp.int32) < live_tiles * TILE
    return jnp.where(live_rows[:, None], attention, 0.0).astype(jnp.bfloat16)


def reference(tree_queries, tree_keys, tree_values, cache_keys, cache_values, sinks, parents, tile_counts, out_weight):
    weight_groups = out_weight.astype(jnp.float32).reshape(N_TP, HEADS * HEAD_DIM // N_TP, D)

    def per_request(operands):
        queries, keys_tree, values_tree, keys_cache, values_cache, parent_row, live_tiles = operands
        attention = request_attention(queries, keys_tree, values_tree, keys_cache, values_cache, sinks, parent_row, live_tiles)
        pieces = attention.astype(jnp.float32).reshape(TREE, N_TP, HEADS * HEAD_DIM // N_TP)
        partial_value = jnp.einsum("tnh,nhd->ntd", pieces, weight_groups).astype(jnp.bfloat16)
        partial_value = lax.optimization_barrier(partial_value)
        return partial_value.astype(jnp.float32).sum(0).astype(jnp.bfloat16)

    return lax.map(per_request, (tree_queries, tree_keys, tree_values, cache_keys, cache_values, parents, tile_counts))
```

```python
import jax
import jax.numpy as jnp
from jax import lax
from jax.experimental import pallas as pl
from jax.experimental.pallas import tpu as pltpu
from jax.sharding import Mesh
from jax.sharding import PartitionSpec as P

HEADS = 64
KV_HEADS = 8
HEAD_DIM = 64
TREE = 512
TILE = 128
CTX = 1024
N_Y, N_X, N_ZL, N_ZH, N_CORE = 8, 4, 2, 4, 2
COLS = 45
PAD = 48
CUT = 16
K_DEV = 512
CHUNK_ROWS = ((0, 1), (-1, 2), (-2, 3), (-3, 4))
CHUNK = 2 * N_X * PAD
HALF = TILE // 2
masked_score = -1e30
MESH = pl.DeviceIdType.MESH
REQ = ("y", "x", "zl")
TP = ("zh", "core")
F32 = jnp.float32
BF16 = jnp.bfloat16


def nt(a, b):
    return lax.dot_general(a, b, (((1,), (1,)), ((), ())), preferred_element_type=F32)


def nn(a, b):
    return jnp.dot(a, b, preferred_element_type=F32)


def ids(shape, dim):
    return lax.broadcasted_iota(jnp.int32, shape, dim)


ROW_OFFSETS = (0, 1, -1, 2, -2, 3, -3, 4)
NAMES = (
    ["s0", "s1"]
    + ["ax" + k for k in "PMF"]
    + ["ay%d" % r for r in ROW_OFFSETS[1:]]
    + ["by%d" % r for r in ROW_OFFSETS[1:]]
    + ["bx%d%s" % (r, k) for r in ROW_OFFSETS for k in "PMF"]
    + ["at%d" % t for t in range(4)]
    + ["rs%d%d" % (c, k) for c in range(4) for k in range(6)]
    + ["fi%d" % c for c in range(4)]
)
INDEX = {name: i for i, name in enumerate(NAMES)}


def kernel(
    q_ref, tk_ref, tv_ref, ck_ref, cv_ref, sink_ref, par_ref, cnt_ref, w_ref,
    out_ref,
    wt, wg, k2, vx, bias, reach, att, snd, rcv, fin, hrecv, sel,
    send_sem, recv_sem, local_sem,
):
    y, x, zl = lax.axis_index("y"), lax.axis_index("x"), lax.axis_index("zl")
    zh, core = lax.axis_index("zh"), lax.axis_index("core")
    d = 1 - 2 * core

    def wrap(a, n):
        return lax.rem(a + n, n)

    xp, xm, xd = ({"x": wrap(x + s, N_X)} for s in (1, -1, d))
    yp, ym, yd = ({"y": wrap(y + s, N_Y)} for s in (1, -1, d))
    zp, zm = ({"zh": wrap(zh + s, N_ZH)} for s in (1, -1))
    partner = {"core": 1 - core}

    barrier = pltpu.get_barrier_semaphore()
    peers = [partner, xp, xm, yp, ym, zp, zm]
    peers += [{"zl": 1 - zl, "core": 0}, {"zl": 1 - zl, "core": 1}]
    for peer in peers:
        pl.semaphore_signal(barrier, inc=1, device_id=peer, device_id_type=MESH)

    pick = (ids((PAD, COLS), 0) == ids((PAD, COLS), 1)).astype(F32).astype(BF16)
    wt[...] = nt(pick, w_ref[...]).astype(BF16)
    pl.semaphore_wait(barrier, len(peers))

    started = []

    def copy(name, src, dst, device):
        i = INDEX[name]
        return pltpu.make_async_remote_copy(
            src_ref=src, dst_ref=dst, send_sem=send_sem.at[i], recv_sem=recv_sem.at[i],
            device_id=device, device_id_type=MESH,
        )

    def send(name, src, dst, device):
        one = copy(name, src, dst, device)
        one.start()
        started.append(one)

    def await_recv(name, dst):
        copy(name, dst, dst, partner).wait_recv()

    def slot(xx, yy):
        return 4 * wrap(yy, N_Y) + wrap(xx, N_X)

    own = slot(x, y)

    def lanes(k):
        return pl.ds(pl.multiple_of(k * K_DEV, K_DEV), K_DEV)

    mine = wg.at[own, :, lanes(core)]
    far = pltpu.make_async_remote_copy(
        src_ref=wt, dst_ref=mine, send_sem=send_sem.at[INDEX["s0"]],
        recv_sem=recv_sem.at[core], device_id={"zl": 1 - zl, "core": zl}, device_id_type=MESH,
    )
    far.start()
    near = pltpu.make_async_remote_copy(
        src_ref=wt, dst_ref=mine, send_sem=send_sem.at[INDEX["s1"]],
        recv_sem=recv_sem.at[core], device_id=partner, device_id_type=MESH,
    )
    here = pltpu.make_async_copy(wt, mine, local_sem)

    @pl.when(zl == core)
    def _():
        here.start()

    @pl.when(zl != core)
    def _():
        near.start()

    def a_block(xx, yy):
        return wg.at[slot(xx, yy), pl.ds(0, CUT), :]

    def a_row(yy):
        return wg.at[pl.ds(4 * wrap(yy, N_Y), 4), pl.ds(0, CUT), :]

    def b_block(xx, yy):
        return wg.at[slot(xx, yy), pl.ds(CUT, PAD - CUT), :]

    messages = {
        "axP": (a_block(x, y), a_block(x - 1, y), xp),
        "axM": (a_block(x, y), a_block(x + 1, y), xm),
        "axF": (a_block(x - d, y), a_block(x + 2, y), xd),
        "ay4": (a_row(y - 3 * d), a_row(y + 4), yd),
        "by4": (b_block(x, y - 3 * d), b_block(x, y + 4), yd),
    }
    for k in (1, 2, 3):
        messages["ay%d" % -k] = (a_row(y - k + 1), a_row(y - k), yp)
        messages["ay%d" % k] = (a_row(y + k - 1), a_row(y + k), ym)
        messages["by%d" % -k] = (b_block(x, y - k + 1), b_block(x, y - k), yp)
        messages["by%d" % k] = (b_block(x, y + k - 1), b_block(x, y + k), ym)
    for r in ROW_OFFSETS:
        messages["bx%dP" % r] = (b_block(x, y + r), b_block(x - 1, y + r), xp)
        messages["bx%dM" % r] = (b_block(x, y + r), b_block(x + 1, y + r), xm)
        messages["bx%dF" % r] = (b_block(x - d, y + r), b_block(x + 2, y + r), xd)

    def go(name):
        src, _, device = messages[name]
        send(name, src, src, device)

    def got(name):
        await_recv(name, messages[name][1])

    def begin_gather():
        for k in range(2):
            part = wg.at[own, :, pl.ds(k * K_DEV, K_DEV)]
            waiting = pltpu.make_async_remote_copy(
                src_ref=part, dst_ref=part, send_sem=send_sem.at[0], recv_sem=recv_sem.at[k],
                device_id=partner, device_id_type=MESH,
            )

            @pl.when((zl != core) | (core != k))
            def _():
                waiting.wait_recv()

        @pl.when(zl == core)
        def _():
            here.wait()

        for name in ("axP", "axM", "by1", "by-1", "bx0P", "bx0M"):
            go(name)

    def row_b(r):
        got("by%d" % r)
        if abs(r) < 3:
            go("by%d" % (r + (1 if r > 0 else -1)))
        go("bx%dP" % r)
        go("bx%dM" % r)

    def last_hop(kind):
        go("%sy4" % kind)

    def relay(r):
        got("bx%dP" % r)
        got("bx%dM" % r)
        go("bx%dF" % r)

    def row_a(r):
        got("ay%d" % r)
        if abs(r) < 3:
            go("ay%d" % (r + (1 if r > 0 else -1)))

    def g1():
        got("axP")
        got("axM")
        go("axF")

    def g2():
        row_b(1)
        row_b(-1)
        relay(0)

    def g3():
        got("axF")
        go("ay1")
        go("ay-1")

    def g4():
        row_b(2)
        row_b(-2)
        relay(1)
        relay(-1)

    def g5():
        row_a(1)
        row_a(-1)

    def g6():
        row_b(3)
        row_b(-3)
        last_hop("b")
        relay(2)
        relay(-2)

    def g7():
        row_a(2)
        row_a(-2)

    def g8():
        got("by4")
        go("bx4P")
        go("bx4M")
        relay(3)
        relay(-3)

    def g9():
        row_a(3)
        row_a(-3)
        last_hop("a")

    def g10():
        relay(4)

    def chunk_ready(c):
        for r in CHUNK_ROWS[c]:
            got("bx%dF" % r)
        if 4 in CHUNK_ROWS[c]:
            got("ay4")

    eye_k = (ids((HEAD_DIM, 2 * HEAD_DIM), 0) == ids((HEAD_DIM, 2 * HEAD_DIM), 1) % HEAD_DIM).astype(F32).astype(BF16)
    eye_v = (ids((HEAD_DIM, 2 * HEAD_DIM), 0) == ids((HEAD_DIM, 2 * HEAD_DIM), 1)).astype(F32).astype(BF16)
    ones_v = (ids((1, 2 * HEAD_DIM), 1) >= HEAD_DIM).astype(F32)
    for source, at, length in ((ck_ref, 0, CTX), (tk_ref, CTX, TREE)):
        k2[pl.ds(at, length), :] = nn(source[...], eye_k).astype(BF16)
    for source, at, length in ((cv_ref, 0, CTX), (tv_ref, CTX, TREE)):
        vx[pl.ds(at, length), :] = (nn(source[...], eye_v) + ones_v).astype(BF16)

    begin_gather()

    square = (TREE, TREE)
    eye = (ids(square, 0) == ids(square, 1)).astype(F32).astype(BF16)
    up = ((ids(square, 0) == par_ref[...]) | (ids(square, 0) == ids(square, 1))).astype(F32).astype(BF16)
    reach[...] = nt(eye, up).astype(BF16)

    def squaring(_, carry):
        twice = nn(reach[...], reach[...])
        reach[...] = (twice > 0.5).astype(F32).astype(BF16)
        return carry

    lax.fori_loop(0, 4, squaring, 0)
    g1()
    lax.fori_loop(0, 5, squaring, 0)
    bias[...] = jnp.where(reach[...].astype(F32) > 0.5, 0.0, masked_score)
    g2()
    g3()

    low = ids((TILE, TILE), 1) < HEAD_DIM
    live_tiles = cnt_ref[0]

    def tile_rows(t):
        return pl.ds(pl.multiple_of(t * TILE, TILE), TILE)

    def attend(t, n):
        rows = tile_rows(t)

        def pair(p, carry):
            columns = pl.ds(pl.multiple_of(p * TILE, TILE), TILE)
            both = q_ref[rows, columns].astype(F32) * (HEAD_DIM**-0.5)
            q2 = jnp.concatenate(
                [jnp.where(low, both, 0.0), jnp.where(low, 0.0, both)], axis=0
            ).astype(BF16)
            s_c = nt(q2, k2[pl.ds(0, CTX), :])
            mask = bias[rows, :]
            s_t = nt(q2, k2[pl.ds(CTX, TREE), :]) + jnp.concatenate([mask, mask], axis=0)
            first = ids((2 * TILE, 1), 0) < TILE
            sink = jnp.where(first, sink_ref[2 * p], sink_ref[2 * p + 1])
            peak = jnp.maximum(
                jnp.maximum(s_c.max(-1, keepdims=True), s_t.max(-1, keepdims=True)), sink
            )
            p_c = jnp.exp(s_c - peak).astype(BF16)
            p_t = jnp.exp(s_t - peak).astype(BF16)
            o = nn(p_c, vx[pl.ds(0, CTX), :]) + nn(p_t, vx[pl.ds(CTX, TREE), :])
            den = pltpu.roll(o, HEAD_DIM, 1) + jnp.exp(sink - peak)
            res = o / den
            odd = pltpu.roll(res[TILE:], HEAD_DIM, 1)
            res = jnp.where(low, res[:TILE], odd)
            res = jnp.where(t < live_tiles, res, 0.0)
            att[core, rows, columns] = res.astype(BF16)
            return carry

        lax.fori_loop(0, 4, pair, 0)
        part = att.at[core, rows, :]
        send("at%d" % n, part, part, partner)

    opp, up_t, dn_t = wrap(zh + 2, N_ZH), wrap(zh + 1, N_ZH), wrap(zh - 1, N_ZH)
    tiles = (opp, up_t, dn_t, zh)

    def att_ready(n):
        await_recv("at%d" % n, att.at[1 - core, tile_rows(tiles[n]), :])

    attend(opp, 0)
    g4()
    g5()
    attend(up_t, 1)
    g6()
    g7()
    attend(dn_t, 2)
    g8()
    g9()
    attend(zh, 3)
    g10()

    shape = (CHUNK, CHUNK)
    lane, column = ids(shape, 0), ids(shape, 1)
    for hf in range(2):
        inner = lane - hf * N_X * PAD
        block = sum((inner >= PAD * i).astype(jnp.int32) for i in (1, 2, 3))
        j = inner - PAD * block
        inside = (inner >= 0) & (inner < N_X * PAD) & (j < COLS)
        for z in range(N_ZL):
            hit = inside & (column == COLS * (2 * block + z) + j)
            sel[hf, z] = hit.astype(F32).astype(BF16)

    for n in range(4):
        att_ready(n)

    def project(t, c):
        a, b = CHUNK_ROWS[c]
        wa = wg[pl.ds(4 * wrap(y + a, N_Y), 4)].reshape(N_X * PAD, 2 * K_DEV)
        wb = wg[pl.ds(4 * wrap(y + b, N_Y), 4)].reshape(N_X * PAD, 2 * K_DEV)
        w = jnp.concatenate([wa, wb], axis=0)
        rows = tile_rows(t)
        return nt(att[0, rows, :], w[:, :K_DEV]) + nt(att[1, rows, :], w[:, K_DEV:])

    def ship(c, k, value, device):
        snd[c, k] = value.astype(BF16)
        send("rs%d%d" % (c, k), snd.at[c, k], rcv.at[c, k], device)

    def landed(c, k):
        await_recv("rs%d%d" % (c, k), rcv.at[c, k])
        return rcv[c, k].astype(F32)

    kept = {}

    def phase1(c):
        chunk_ready(c)
        value = project(opp, c)
        ship(c, 0, value[:HALF], zp)
        ship(c, 1, value[HALF:], zm)
        value = project(up_t, c)
        ship(c, 2, value[HALF:], zp)
        fin[0, c] = value[:HALF]
        value = project(dn_t, c)
        ship(c, 3, value[:HALF], zm)
        fin[1, c] = value[HALF:]

    def phase2(c):
        ship(c, 4, fin[0, c] + landed(c, 0), zp)
        ship(c, 5, fin[1, c] + landed(c, 1), zm)
        value = project(zh, c)
        fin[0, c] = value[:HALF]
        fin[1, c] = value[HALF:]

    def phase3(c):
        top = fin[0, c] + landed(c, 4) + landed(c, 3)
        low_half = fin[1, c] + landed(c, 5) + landed(c, 2)
        keep = jnp.where(core == 0, top, low_half).astype(BF16)
        give = jnp.where(core == 0, low_half, top).astype(BF16)
        hrecv[0, c] = keep
        hrecv[1, c] = give
        send("fi%d" % c, hrecv.at[1, c], hrecv.at[2, c], partner)

    def phase4(c):
        await_recv("fi%d" % c, hrecv.at[2, c])
        for hf in range(2):
            r = nn(hrecv[0, c], sel[hf, core]) + nn(hrecv[2, c], sel[hf, 1 - core])
            out_ref[wrap(y + CHUNK_ROWS[c][hf], N_Y)] = r[:, : N_X * 2 * COLS].astype(BF16)

    phase1(0)
    phase1(1)
    phase2(0)
    phase1(2)
    phase2(1)
    phase1(3)
    phase2(2)
    phase3(0)
    phase2(3)
    phase3(1)
    phase4(0)
    phase3(2)
    phase4(1)
    phase3(3)
    phase4(2)
    phase4(3)

    for one in started:
        one.wait_send()
    far.wait_send()

    @pl.when(zl != core)
    def _():
        near.wait_send()


def per_device(
    tree_queries, tree_keys, tree_values, cache_keys, cache_values, sinks, parents, tile_counts, out_weight
):
    vmem = pl.BlockSpec(memory_space=pltpu.VMEM)
    smem = pl.BlockSpec(memory_space=pltpu.SMEM)
    keys = CTX + TREE
    count = len(NAMES)
    out = pl.pallas_call(
        kernel,
        out_shape=jax.ShapeDtypeStruct((N_Y, HALF, N_X * 2 * COLS), BF16),
        in_specs=[vmem, vmem, vmem, vmem, vmem, smem, vmem, smem, vmem],
        out_specs=vmem,
        scratch_shapes=[
            pltpu.VMEM((PAD, K_DEV), BF16),
            pltpu.VMEM((N_Y * N_X, PAD, 2 * K_DEV), BF16),
            pltpu.VMEM((keys, 2 * HEAD_DIM), BF16),
            pltpu.VMEM((keys, 2 * HEAD_DIM), BF16),
            pltpu.VMEM((TREE, TREE), F32),
            pltpu.VMEM((TREE, TREE), BF16),
            pltpu.VMEM((2, TREE, K_DEV), BF16),
            pltpu.VMEM((4, 6, HALF, CHUNK), BF16),
            pltpu.VMEM((4, 6, HALF, CHUNK), BF16),
            pltpu.VMEM((2, 4, HALF, CHUNK), F32),
            pltpu.VMEM((3, 4, HALF, CHUNK), BF16),
            pltpu.VMEM((2, 2, CHUNK, CHUNK), BF16),
            pltpu.SemaphoreType.DMA((count,)),
            pltpu.SemaphoreType.DMA((count,)),
            pltpu.SemaphoreType.DMA,
        ],
        compiler_params=pltpu.CompilerParams(collective_id=0, has_side_effects=True),
    )(
        tree_queries[0], tree_keys[0], tree_values[0], cache_keys[0], cache_values[0],
        sinks, parents, tile_counts, out_weight,
    )
    return out.transpose(1, 0, 2).reshape(1, HALF, -1)


def solution(mesh):
    sizes = (N_Y, N_X, N_ZL, N_ZH, N_CORE)
    split = Mesh(mesh.devices.reshape(sizes), (*REQ, *TP))
    placed = (
        P(REQ, None, TP),
        P(REQ, None, TP),
        P(REQ, None, TP),
        P(REQ, None, TP),
        P(REQ, None, TP),
        P(TP),
        P(REQ, None),
        P(REQ),
        P(TP, REQ),
    )
    return jax.shard_map(
        per_device, mesh=split, in_specs=placed, out_specs=P(REQ, TP, None), check_vma=False
    )
```

```python
import jax
import jax.numpy as jnp
from jax import lax
from jax.experimental import pallas as pl
from jax.experimental.pallas import tpu as pltpu
from jax.sharding import Mesh
from jax.sharding import PartitionSpec as P

HEADS = 64
KV_HEADS = 8
HEAD_DIM = 64
TREE = 512
TILE = 128
CTX = 1024
N_Y, N_X, N_ZL, N_ZH, N_CORE = 8, 4, 2, 4, 2
COLS = 45
PAD = 48
CUT = 16
K_DEV = 512
CHUNK_ROWS = ((0, 1), (-1, 2), (-2, 3), (-3, 4))
CHUNK = 2 * N_X * PAD
HALF = TILE // 2
BLOCK = TREE // 2
VROWS = HEAD_DIM + 16
masked_score = -1e30
MESH = pl.DeviceIdType.MESH
REQ = ("y", "x", "zl")
TP = ("zh", "core")
F32 = jnp.float32
BF16 = jnp.bfloat16


def nt(a, b):
    return lax.dot_general(a, b, (((1,), (1,)), ((), ())), preferred_element_type=F32)


def nn(a, b):
    return jnp.dot(a, b, preferred_element_type=F32)


def ids(shape, dim):
    return lax.broadcasted_iota(jnp.int32, shape, dim)


ROW_OFFSETS = (0, 1, -1, 2, -2, 3, -3, 4)
NAMES = (
    ["s0", "s1"]
    + ["ax" + k for k in "PMF"]
    + ["ay%d" % r for r in ROW_OFFSETS[1:]]
    + ["by%d" % r for r in ROW_OFFSETS[1:]]
    + ["bx%d%s" % (r, k) for r in ROW_OFFSETS for k in "PMF"]
    + ["at%d" % t for t in range(4)]
    + ["rs%d%d" % (c, k) for c in range(4) for k in range(6)]
    + ["fi%d" % c for c in range(4)]
)
INDEX = {name: i for i, name in enumerate(NAMES)}


def kernel(
    q_ref, tk_ref, tv_ref, ck_ref, cv_ref, sink_ref, par_ref, cnt_ref, w_ref,
    out_ref,
    wt, wg, k2, vx, bias, reach, att, snd, rcv, fin, hrecv, sel, res_rows,
    send_sem, recv_sem, local_sem,
):
    y, x, zl = lax.axis_index("y"), lax.axis_index("x"), lax.axis_index("zl")
    zh, core = lax.axis_index("zh"), lax.axis_index("core")
    d = 1 - 2 * core

    def wrap(a, n):
        return lax.rem(a + n, n)

    xp, xm, xd = ({"x": wrap(x + s, N_X)} for s in (1, -1, d))
    yp, ym, yd = ({"y": wrap(y + s, N_Y)} for s in (1, -1, d))
    zp, zm = ({"zh": wrap(zh + s, N_ZH)} for s in (1, -1))
    partner = {"core": 1 - core}

    barrier = pltpu.get_barrier_semaphore()
    peers = [partner, xp, xm, yp, ym, zp, zm]
    peers += [{"zl": 1 - zl, "core": 0}, {"zl": 1 - zl, "core": 1}]
    for peer in peers:
        pl.semaphore_signal(barrier, inc=1, device_id=peer, device_id_type=MESH)

    block = w_ref[...].astype(F32)
    wt[...] = jnp.concatenate([block, jnp.zeros((PAD - COLS, K_DEV), F32)], axis=0).astype(BF16)
    pl.semaphore_wait(barrier, len(peers))

    started = []

    def copy(name, src, dst, device):
        i = INDEX[name]
        return pltpu.make_async_remote_copy(
            src_ref=src, dst_ref=dst, send_sem=send_sem.at[i], recv_sem=recv_sem.at[i],
            device_id=device, device_id_type=MESH,
        )

    def send(name, src, dst, device):
        one = copy(name, src, dst, device)
        one.start()
        started.append(one)

    def await_recv(name, dst):
        copy(name, dst, dst, partner).wait_recv()

    def slot(xx, yy):
        return 4 * wrap(yy, N_Y) + wrap(xx, N_X)

    own = slot(x, y)

    def lanes(k):
        return pl.ds(pl.multiple_of(k * K_DEV, K_DEV), K_DEV)

    mine = wg.at[own, :, lanes(core)]
    far = pltpu.make_async_remote_copy(
        src_ref=wt, dst_ref=mine, send_sem=send_sem.at[INDEX["s0"]],
        recv_sem=recv_sem.at[core], device_id={"zl": 1 - zl, "core": zl}, device_id_type=MESH,
    )
    far.start()
    near = pltpu.make_async_remote_copy(
        src_ref=wt, dst_ref=mine, send_sem=send_sem.at[INDEX["s1"]],
        recv_sem=recv_sem.at[core], device_id=partner, device_id_type=MESH,
    )
    here = pltpu.make_async_copy(wt, mine, local_sem)

    @pl.when(zl == core)
    def _():
        here.start()

    @pl.when(zl != core)
    def _():
        near.start()

    def a_block(xx, yy):
        return wg.at[slot(xx, yy), pl.ds(0, CUT), :]

    def a_row(yy):
        return wg.at[pl.ds(4 * wrap(yy, N_Y), 4), pl.ds(0, CUT), :]

    def b_block(xx, yy):
        return wg.at[slot(xx, yy), pl.ds(CUT, PAD - CUT), :]

    messages = {
        "axP": (a_block(x, y), a_block(x - 1, y), xp),
        "axM": (a_block(x, y), a_block(x + 1, y), xm),
        "axF": (a_block(x - d, y), a_block(x + 2, y), xd),
        "ay4": (a_row(y - 3 * d), a_row(y + 4), yd),
        "by4": (b_block(x, y - 3 * d), b_block(x, y + 4), yd),
    }
    for k in (1, 2, 3):
        messages["ay%d" % -k] = (a_row(y - k + 1), a_row(y - k), yp)
        messages["ay%d" % k] = (a_row(y + k - 1), a_row(y + k), ym)
        messages["by%d" % -k] = (b_block(x, y - k + 1), b_block(x, y - k), yp)
        messages["by%d" % k] = (b_block(x, y + k - 1), b_block(x, y + k), ym)
    for r in ROW_OFFSETS:
        messages["bx%dP" % r] = (b_block(x, y + r), b_block(x - 1, y + r), xp)
        messages["bx%dM" % r] = (b_block(x, y + r), b_block(x + 1, y + r), xm)
        messages["bx%dF" % r] = (b_block(x - d, y + r), b_block(x + 2, y + r), xd)

    def go(name):
        src, _, device = messages[name]
        send(name, src, src, device)

    def got(name):
        await_recv(name, messages[name][1])

    def begin_gather():
        for k in range(2):
            part = wg.at[own, :, pl.ds(k * K_DEV, K_DEV)]
            waiting = pltpu.make_async_remote_copy(
                src_ref=part, dst_ref=part, send_sem=send_sem.at[0], recv_sem=recv_sem.at[k],
                device_id=partner, device_id_type=MESH,
            )

            @pl.when((zl != core) | (core != k))
            def _():
                waiting.wait_recv()

        @pl.when(zl == core)
        def _():
            here.wait()

        for name in ("axP", "axM", "by1", "by-1", "bx0P", "bx0M"):
            go(name)

    def row_b(r):
        got("by%d" % r)
        if abs(r) < 3:
            go("by%d" % (r + (1 if r > 0 else -1)))
        go("bx%dP" % r)
        go("bx%dM" % r)

    def last_hop(kind):
        go("%sy4" % kind)

    def relay(r):
        got("bx%dP" % r)
        got("bx%dM" % r)
        go("bx%dF" % r)

    def row_a(r):
        got("ay%d" % r)
        if abs(r) < 3:
            go("ay%d" % (r + (1 if r > 0 else -1)))

    def g1():
        got("axP")
        got("axM")
        go("axF")

    def g3():
        got("axF")
        go("ay1")
        go("ay-1")

    def g5():
        row_a(1)
        row_a(-1)

    def g6():
        row_b(3)
        row_b(-3)
        last_hop("b")
        relay(2)
        relay(-2)

    def g7():
        row_a(2)
        row_a(-2)

    def g8():
        got("by4")
        go("bx4P")
        go("bx4M")
        relay(3)
        relay(-3)

    def g9():
        row_a(3)
        row_a(-3)
        last_hop("a")

    def g10():
        relay(4)

    def chunk_ready(c):
        for r in CHUNK_ROWS[c]:
            got("bx%dF" % r)
        if 4 in CHUNK_ROWS[c]:
            got("ay4")

    for source, at, length in ((ck_ref, 0, CTX), (tk_ref, CTX, TREE)):
        keys = source[...].astype(F32)
        k2[pl.ds(at, length), :] = jnp.concatenate([keys, keys], axis=0).T.astype(BF16)
    vx[pl.ds(0, HEAD_DIM), pl.ds(0, CTX)] = cv_ref[...]
    vx[pl.ds(0, HEAD_DIM), pl.ds(CTX, TREE)] = tv_ref[...]
    vx[pl.ds(HEAD_DIM, VROWS - HEAD_DIM), :] = jnp.ones((VROWS - HEAD_DIM, CTX + TREE), BF16)

    square = (BLOCK, BLOCK)

    def parent_of(j0, i0):
        return (ids(square, 0) + j0) == par_ref[:, pl.ds(i0, BLOCK)]

    for i in range(2):
        edge = parent_of(i * BLOCK, i * BLOCK) | (ids(square, 0) == ids(square, 1))
        reach[i] = edge.astype(F32).astype(BF16)

    begin_gather()

    def squaring(_, carry):
        twice = [nn(reach[i], reach[i]) for i in range(2)]
        for i in range(2):
            reach[i] = (twice[i] > 0.5).astype(F32).astype(BF16)
        return carry

    lax.fori_loop(0, 4, squaring, 0)
    g1()
    lax.fori_loop(0, 4, squaring, 0)
    across = nn(reach[0], parent_of(0, BLOCK).astype(F32).astype(BF16)).astype(BF16)
    across = nn(across, reach[1])

    def as_bias(seen):
        return jnp.where(seen.astype(F32) > 0.5, 0.0, masked_score)

    bias[pl.ds(0, BLOCK), pl.ds(0, BLOCK)] = as_bias(reach[0])
    bias[pl.ds(0, BLOCK), pl.ds(BLOCK, BLOCK)] = as_bias(across)
    bias[pl.ds(BLOCK, BLOCK), pl.ds(0, BLOCK)] = jnp.full(square, masked_score, F32)
    bias[pl.ds(BLOCK, BLOCK), pl.ds(BLOCK, BLOCK)] = as_bias(reach[1])

    low = ids((TILE, TILE), 1) < HEAD_DIM
    live_tiles = cnt_ref[0]

    def tile_rows(t):
        return pl.ds(pl.multiple_of(t * TILE, TILE), TILE)

    def attend(t, n, half):
        rows = tile_rows(t)
        mask = bias[:, rows]
        mask = jnp.concatenate([mask, mask], axis=1)
        for p in (2 * half, 2 * half + 1):
            columns = pl.ds(p * TILE, TILE)
            both = q_ref[rows, columns].astype(F32) * (HEAD_DIM**-0.5)
            q2 = jnp.concatenate(
                [jnp.where(low, both, 0.0), jnp.where(low, 0.0, both)], axis=0
            ).astype(BF16)
            s_c = nt(k2[pl.ds(0, CTX), :], q2)
            s_t = nt(k2[pl.ds(CTX, TREE), :], q2) + mask
            first = ids((1, 2 * TILE), 1) < TILE
            sink = jnp.where(first, sink_ref[2 * p], sink_ref[2 * p + 1])
            peak = jnp.maximum(
                jnp.maximum(s_c.max(0, keepdims=True), s_t.max(0, keepdims=True)), sink
            )
            p_c = jnp.exp(s_c - peak).astype(BF16)
            p_t = jnp.exp(s_t - peak).astype(BF16)
            o = nn(vx[:, pl.ds(0, CTX)], p_c) + nn(vx[:, pl.ds(CTX, TREE)], p_t)
            den = o[HEAD_DIM : HEAD_DIM + 1] + jnp.exp(sink - peak)
            res = o[:HEAD_DIM] / den
            res = jnp.concatenate([res[:, :TILE], res[:, TILE:]], axis=0).T
            res = jnp.where(t < live_tiles, res, 0.0)
            att[core, rows, columns] = res.astype(BF16)
        if half:
            part = att.at[core, rows, :]
            send("at%d" % n, part, part, partner)

    opp, up_t, dn_t = wrap(zh + 2, N_ZH), wrap(zh + 1, N_ZH), wrap(zh - 1, N_ZH)
    tiles = (opp, up_t, dn_t, zh)

    def att_ready(n):
        await_recv("at%d" % n, att.at[1 - core, tile_rows(tiles[n]), :])

    attend(opp, 0, 0)
    row_b(1)
    row_b(-1)
    attend(opp, 0, 1)
    relay(0)
    attend(up_t, 1, 0)
    g3()
    attend(up_t, 1, 1)
    row_b(2)
    row_b(-2)
    attend(dn_t, 2, 0)
    relay(1)
    relay(-1)
    attend(dn_t, 2, 1)
    g5()
    attend(zh, 3, 0)
    g6()
    attend(zh, 3, 1)

    shape = (CHUNK, CHUNK)
    lane, column = ids(shape, 0), ids(shape, 1)
    for hf in range(2):
        inner = lane - hf * N_X * PAD
        block = sum((inner >= PAD * i).astype(jnp.int32) for i in (1, 2, 3))
        j = inner - PAD * block
        inside = (inner >= 0) & (inner < N_X * PAD) & (j < COLS)
        for z in range(N_ZL):
            hit = inside & (column == COLS * (2 * block + z) + j)
            sel[hf, z] = hit.astype(F32).astype(BF16)

    for n in range(4):
        att_ready(n)

    def project(t, c):
        a, b = CHUNK_ROWS[c]
        wa = wg[pl.ds(4 * wrap(y + a, N_Y), 4)].reshape(N_X * PAD, 2 * K_DEV)
        wb = wg[pl.ds(4 * wrap(y + b, N_Y), 4)].reshape(N_X * PAD, 2 * K_DEV)
        w = jnp.concatenate([wa, wb], axis=0)
        rows = tile_rows(t)
        return nt(att[0, rows, :], w[:, :K_DEV]) + nt(att[1, rows, :], w[:, K_DEV:])

    def ship(c, k, value, device):
        snd[c, k] = value.astype(BF16)
        send("rs%d%d" % (c, k), snd.at[c, k], rcv.at[c, k], device)

    def landed(c, k):
        await_recv("rs%d%d" % (c, k), rcv.at[c, k])
        return rcv[c, k].astype(F32)

    kept = {}

    def phase1(c):
        chunk_ready(c)
        value = project(opp, c)
        ship(c, 0, value[:HALF], zp)
        ship(c, 1, value[HALF:], zm)
        value = project(up_t, c)
        ship(c, 2, value[HALF:], zp)
        fin[0, c] = value[:HALF]
        value = project(dn_t, c)
        ship(c, 3, value[:HALF], zm)
        fin[1, c] = value[HALF:]

    def phase2(c):
        ship(c, 4, fin[0, c] + landed(c, 0), zp)
        ship(c, 5, fin[1, c] + landed(c, 1), zm)
        value = project(zh, c)
        fin[0, c] = value[:HALF]
        fin[1, c] = value[HALF:]

    def phase3(c):
        top = fin[0, c] + landed(c, 4) + landed(c, 3)
        low_half = fin[1, c] + landed(c, 5) + landed(c, 2)
        keep = jnp.where(core == 0, top, low_half).astype(BF16)
        give = jnp.where(core == 0, low_half, top).astype(BF16)
        hrecv[0, c] = keep
        hrecv[1, c] = give
        send("fi%d" % c, hrecv.at[1, c], hrecv.at[2, c], partner)

    def phase4(c):
        await_recv("fi%d" % c, hrecv.at[2, c])
        for hf in range(2):
            r = nn(hrecv[0, c], sel[hf, core]) + nn(hrecv[2, c], sel[hf, 1 - core])
            res_rows[wrap(y + CHUNK_ROWS[c][hf], N_Y)] = r.astype(BF16)

    phase1(0)
    g7()
    phase1(1)
    phase2(0)
    g8()
    g9()
    phase1(2)
    phase2(1)
    g10()
    phase1(3)
    phase2(2)
    phase3(0)
    phase2(3)
    phase3(1)
    phase4(0)
    phase3(2)
    phase4(1)
    phase3(3)
    phase4(2)
    phase4(3)
    width = N_X * 2 * COLS
    for i in range(N_Y):
        out_ref[:, pl.ds(width * i, width)] = res_rows[i][:, :width]

    for one in started:
        one.wait_send()
    far.wait_send()

    @pl.when(zl != core)
    def _():
        near.wait_send()


def per_device(
    tree_queries, tree_keys, tree_values, cache_keys, cache_values, sinks, parents, tile_counts, out_weight
):
    vmem = pl.BlockSpec(memory_space=pltpu.VMEM)
    smem = pl.BlockSpec(memory_space=pltpu.SMEM)
    keys = CTX + TREE
    count = len(NAMES)
    out = pl.pallas_call(
        kernel,
        out_shape=jax.ShapeDtypeStruct((HALF, N_Y * N_X * 2 * COLS), BF16),
        in_specs=[vmem, vmem, vmem, vmem, vmem, smem, vmem, smem, vmem],
        out_specs=vmem,
        scratch_shapes=[
            pltpu.VMEM((PAD, K_DEV), BF16),
            pltpu.VMEM((N_Y * N_X, PAD, 2 * K_DEV), BF16),
            pltpu.VMEM((keys, 2 * HEAD_DIM), BF16),
            pltpu.VMEM((VROWS, keys), BF16),
            pltpu.VMEM((TREE, TREE), F32),
            pltpu.VMEM((2, BLOCK, BLOCK), BF16),
            pltpu.VMEM((2, TREE, K_DEV), BF16),
            pltpu.VMEM((4, 6, HALF, CHUNK), BF16),
            pltpu.VMEM((4, 6, HALF, CHUNK), BF16),
            pltpu.VMEM((2, 4, HALF, CHUNK), F32),
            pltpu.VMEM((3, 4, HALF, CHUNK), BF16),
            pltpu.VMEM((2, 2, CHUNK, CHUNK), BF16),
            pltpu.VMEM((N_Y, HALF, CHUNK), BF16),
            pltpu.SemaphoreType.DMA((count,)),
            pltpu.SemaphoreType.DMA((count,)),
            pltpu.SemaphoreType.DMA,
        ],
        compiler_params=pltpu.CompilerParams(collective_id=0, has_side_effects=True),
    )(
        tree_queries[0], tree_keys[0].T, tree_values[0].T, cache_keys[0].T, cache_values[0].T,
        sinks, parents, tile_counts, out_weight.T,
    )
    return out[None]


def solution(mesh):
    sizes = (N_Y, N_X, N_ZL, N_ZH, N_CORE)
    split = Mesh(mesh.devices.reshape(sizes), (*REQ, *TP))
    placed = (
        P(REQ, None, TP),
        P(REQ, None, TP),
        P(REQ, None, TP),
        P(REQ, None, TP),
        P(REQ, None, TP),
        P(TP),
        P(REQ, None),
        P(REQ),
        P(TP, REQ),
    )
    return jax.shard_map(
        per_device, mesh=split, in_specs=placed, out_specs=P(REQ, TP, None), check_vma=False
    )
```

```python
import jax
import jax.numpy as jnp
from jax import lax
from jax.experimental import pallas as pl
from jax.experimental.pallas import tpu as pltpu
from jax.sharding import Mesh
from jax.sharding import PartitionSpec as P

HEADS = 64
KV_HEADS = 8
HEAD_DIM = 64
TREE = 512
TILE = 128
CTX = 1024
N_Y, N_X, N_ZL, N_ZH, N_CORE = 8, 4, 2, 4, 2
COLS = 45
PAD = 48
CUT = 16
K_DEV = 512
CHUNK = 2 * N_X * PAD
HALF = TILE // 2
BLOCK = TREE // 2
VROWS = HEAD_DIM + 16
masked_score = -1e30
MESH = pl.DeviceIdType.MESH
REQ = ("y", "x", "zl")
TP = ("zh", "core")
F32 = jnp.float32
BF16 = jnp.bfloat16


def nt(a, b):
    return lax.dot_general(a, b, (((1,), (1,)), ((), ())), preferred_element_type=F32)


def nn(a, b):
    return jnp.dot(a, b, preferred_element_type=F32)


def ids(shape, dim):
    return lax.broadcasted_iota(jnp.int32, shape, dim)


ROW_OFFSETS = (0, 1, -1, 2, -2, 3, -3, 4)
NAMES = (
    ["s0", "s1"]
    + ["ax" + k for k in "PMF"]
    + ["ay%d" % r for r in range(-3, 5) if r]
    + ["by%d" % r for r in range(-3, 5) if r]
    + ["bx%d%s" % (r, k) for r in range(-3, 5) for k in "PMF"]
    + ["at%d" % t for t in range(4)]
    + ["rs%d%d" % (c, k) for c in range(4) for k in range(6)]
    + ["fi%d" % c for c in range(4)]
)
INDEX = {name: i for i, name in enumerate(NAMES)}


def kernel(
    q_ref, tk_ref, tv_ref, ck_ref, cv_ref, sink_ref, par_ref, cnt_ref, w_ref,
    out_ref,
    wt, wg, k2, vx, bias, reach, att, snd, rcv, fin, hrecv, sel, res_rows, score_a, score_b,
    send_sem, recv_sem, local_sem,
):
    y, x, zl = lax.axis_index("y"), lax.axis_index("x"), lax.axis_index("zl")
    zh, core = lax.axis_index("zh"), lax.axis_index("core")
    d = 1 - 2 * core

    def wrap(a, n):
        return lax.rem(a + n, n)

    xp, xm, xd = ({"x": wrap(x + s, N_X)} for s in (1, -1, d))
    yp, ym, yd = ({"y": wrap(y + s, N_Y)} for s in (1, -1, d))
    zp, zm = ({"zh": wrap(zh + s, N_ZH)} for s in (1, -1))
    partner = {"core": 1 - core}

    barrier = pltpu.get_barrier_semaphore()
    peers = [partner, xp, xm, yp, ym, zp, zm]
    peers += [{"zl": 1 - zl, "core": 0}, {"zl": 1 - zl, "core": 1}]
    for peer in peers:
        pl.semaphore_signal(barrier, inc=1, device_id=peer, device_id_type=MESH)

    block = w_ref[...].astype(F32)
    wt[...] = jnp.concatenate([block, jnp.zeros((PAD - COLS, K_DEV), F32)], axis=0).astype(BF16)
    pl.semaphore_wait(barrier, len(peers))

    def copy(i, src, dst, device):
        return pltpu.make_async_remote_copy(
            src_ref=src, dst_ref=dst, send_sem=send_sem.at[i], recv_sem=recv_sem.at[i],
            device_id=device, device_id_type=MESH,
        )

    def await_recv(i, dst):
        copy(i, dst, dst, partner).wait_recv()

    def slot(xx, yy):
        return 4 * wrap(yy, N_Y) + wrap(xx, N_X)

    own = slot(x, y)

    def lanes(k):
        return pl.ds(pl.multiple_of(k * K_DEV, K_DEV), K_DEV)

    mine = wg.at[own, :, lanes(core)]
    far = pltpu.make_async_remote_copy(
        src_ref=wt, dst_ref=mine, send_sem=send_sem.at[INDEX["s0"]],
        recv_sem=recv_sem.at[core], device_id={"zl": 1 - zl, "core": zl}, device_id_type=MESH,
    )
    far.start()
    near = pltpu.make_async_remote_copy(
        src_ref=wt, dst_ref=mine, send_sem=send_sem.at[INDEX["s1"]],
        recv_sem=recv_sem.at[core], device_id=partner, device_id_type=MESH,
    )
    here = pltpu.make_async_copy(wt, mine, local_sem)

    @pl.when(zl == core)
    def _():
        here.start()

    @pl.when(zl != core)
    def _():
        near.start()

    def a_block(xx, yy):
        return wg.at[slot(xx, yy), pl.ds(0, CUT), :]

    def a_row(yy):
        return wg.at[pl.ds(4 * wrap(yy, N_Y), 4), pl.ds(0, CUT), :]

    def b_block(xx, yy):
        return wg.at[slot(xx, yy), pl.ds(CUT, PAD - CUT), :]

    messages = {
        "axP": (a_block(x, y), a_block(x - 1, y), xp),
        "axM": (a_block(x, y), a_block(x + 1, y), xm),
        "axF": (a_block(x - d, y), a_block(x + 2, y), xd),
        "ay4": (a_row(y - 3 * d), a_row(y + 4), yd),
        "by4": (b_block(x, y - 3 * d), b_block(x, y + 4), yd),
    }
    for k in (1, 2, 3):
        messages["ay%d" % -k] = (a_row(y - k + 1), a_row(y - k), yp)
        messages["ay%d" % k] = (a_row(y + k - 1), a_row(y + k), ym)
        messages["by%d" % -k] = (b_block(x, y - k + 1), b_block(x, y - k), yp)
        messages["by%d" % k] = (b_block(x, y + k - 1), b_block(x, y + k), ym)
    for r in ROW_OFFSETS:
        messages["bx%dP" % r] = (b_block(x, y + r), b_block(x - 1, y + r), xp)
        messages["bx%dM" % r] = (b_block(x, y + r), b_block(x + 1, y + r), xm)
        messages["bx%dF" % r] = (b_block(x - d, y + r), b_block(x + 2, y + r), xd)

    def go(name):
        src, _, device = messages[name]
        copy(INDEX[name], src, src, device).start()

    def got(name):
        await_recv(INDEX[name], messages[name][1])

    def begin_gather():
        for k in range(2):
            part = wg.at[own, :, pl.ds(k * K_DEV, K_DEV)]
            waiting = pltpu.make_async_remote_copy(
                src_ref=part, dst_ref=part, send_sem=send_sem.at[0], recv_sem=recv_sem.at[k],
                device_id=partner, device_id_type=MESH,
            )

            @pl.when((zl != core) | (core != k))
            def _():
                waiting.wait_recv()

        @pl.when(zl == core)
        def _():
            here.wait()

        for name in ("axP", "axM", "by1", "by-1", "bx0P", "bx0M"):
            go(name)

    def row_b(r):
        got("by%d" % r)
        if abs(r) < 3:
            go("by%d" % (r + (1 if r > 0 else -1)))
        go("bx%dP" % r)
        go("bx%dM" % r)

    def last_hop(kind):
        go("%sy4" % kind)

    def relay(r):
        got("bx%dP" % r)
        got("bx%dM" % r)
        go("bx%dF" % r)

    def row_a(r):
        got("ay%d" % r)
        if abs(r) < 3:
            go("ay%d" % (r + (1 if r > 0 else -1)))

    def g1():
        got("axP")
        got("axM")
        go("axF")

    def g3():
        got("axF")
        go("ay1")
        go("ay-1")

    def g5():
        row_a(1)
        row_a(-1)

    def g6():
        row_b(3)
        row_b(-3)
        last_hop("b")
        relay(2)
        relay(-2)

    def g7():
        row_a(2)
        row_a(-2)

    def g8():
        got("by4")
        go("bx4P")
        go("bx4M")
        relay(3)
        relay(-3)

    def g9():
        row_a(3)
        row_a(-3)
        last_hop("a")

    def g10():
        relay(4)

    for source, at, length in ((ck_ref, 0, CTX), (tk_ref, CTX, TREE)):
        keys = source[...].astype(F32)
        k2[pl.ds(at, length), :] = jnp.concatenate([keys, keys], axis=0).T.astype(BF16)
    vx[pl.ds(0, HEAD_DIM), pl.ds(0, CTX)] = cv_ref[...]
    vx[pl.ds(0, HEAD_DIM), pl.ds(CTX, TREE)] = tv_ref[...]
    vx[pl.ds(HEAD_DIM, VROWS - HEAD_DIM), :] = jnp.ones((VROWS - HEAD_DIM, CTX + TREE), BF16)

    square = (BLOCK, BLOCK)

    def parent_of(j0, i0):
        return (ids(square, 0) + j0) == par_ref[:, pl.ds(i0, BLOCK)]

    for i in range(2):
        edge = parent_of(i * BLOCK, i * BLOCK) | (ids(square, 0) == ids(square, 1))
        reach[i] = edge.astype(F32).astype(BF16)

    begin_gather()

    def squaring(_, carry):
        twice = [nn(reach[i], reach[i]) for i in range(2)]
        for i in range(2):
            reach[i] = (twice[i] > 0.5).astype(F32).astype(BF16)
        return carry

    lax.fori_loop(0, 4, squaring, 0)
    g1()
    lax.fori_loop(0, 4, squaring, 0)
    across = nn(reach[0], parent_of(0, BLOCK).astype(F32).astype(BF16)).astype(BF16)
    across = nn(across, reach[1])

    def as_bias(seen):
        return jnp.where(seen.astype(F32) > 0.5, 0.0, masked_score)

    bias[pl.ds(0, BLOCK), pl.ds(0, BLOCK)] = as_bias(reach[0])
    bias[pl.ds(0, BLOCK), pl.ds(BLOCK, BLOCK)] = as_bias(across)
    bias[pl.ds(BLOCK, BLOCK), pl.ds(0, BLOCK)] = jnp.full(square, masked_score, F32)
    bias[pl.ds(BLOCK, BLOCK), pl.ds(BLOCK, BLOCK)] = as_bias(reach[1])

    low = ids((TILE, TILE), 1) < HEAD_DIM
    first = ids((1, 2 * TILE), 1) < TILE
    live_tiles = cnt_ref[0]
    opp, up_t, dn_t = wrap(zh + 2, N_ZH), wrap(zh + 1, N_ZH), wrap(zh - 1, N_ZH)

    def tile_at(n):
        shift = jnp.where(n == 0, 2, jnp.where(n == 1, 1, jnp.where(n == 2, 3, 0)))
        return lax.rem(zh + shift, N_ZH)

    def tile_rows(t):
        return pl.ds(pl.multiple_of(t * TILE, TILE), TILE)

    def columns_of(u):
        return pl.ds(pl.multiple_of(lax.rem(u, 4) * TILE, TILE), TILE)

    def sink_of(u):
        p = lax.rem(u, 4)
        return jnp.where(first, sink_ref[2 * p], sink_ref[2 * p + 1])

    def scores(u, store):
        rows = tile_rows(tile_at(u // 4))
        both = q_ref[rows, columns_of(u)].astype(F32) * (HEAD_DIM**-0.5)
        q2 = jnp.concatenate(
            [jnp.where(low, both, 0.0), jnp.where(low, 0.0, both)], axis=0
        ).astype(BF16)
        top = None
        for i in range((CTX + TREE) // BLOCK):
            s = nt(k2[pl.ds(i * BLOCK, BLOCK), :], q2)
            if i * BLOCK >= CTX:
                mask = bias[pl.ds(i * BLOCK - CTX, BLOCK), rows]
                s = s + jnp.concatenate([mask, mask], axis=1)
            store[pl.ds(i * BLOCK, BLOCK), :] = s
            part = s.reshape(BLOCK // 8, 8, 2 * TILE).max(0)
            top = part if top is None else jnp.maximum(top, part)
        return jnp.maximum(top.max(0, keepdims=True), sink_of(u))

    def weigh(u, store, peak):
        t = tile_at(u // 4)
        o = None
        for i in range((CTX + TREE) // BLOCK):
            keys = pl.ds(i * BLOCK, BLOCK)
            p = jnp.exp(store[keys, :] - peak).astype(BF16)
            part = nn(vx[:, keys], p)
            o = part if o is None else o + part
        den = o[HEAD_DIM : HEAD_DIM + 1] + jnp.exp(sink_of(u) - peak)
        res = o[:HEAD_DIM] / den
        res = jnp.concatenate([res[:, :TILE], res[:, TILE:]], axis=0).T
        res = jnp.where(t < live_tiles, res, 0.0)
        att[core, tile_rows(t), columns_of(u)] = res.astype(BF16)

    def att_copy(n):
        part = att.at[core, tile_rows(tile_at(n)), :]
        return copy(INDEX["at0"] + n, part, part, partner)

    def att_ready(n):
        await_recv(INDEX["at0"] + n, att.at[1 - core, tile_rows(tile_at(n)), :])

    def step_1():
        row_b(1)
        row_b(-1)

    def step_2():
        relay(0)

    def step_4():
        row_b(2)
        row_b(-2)
        relay(1)
        relay(-1)

    events = {0: step_1, 1: step_2, 2: g3, 4: step_4, 6: g5, 7: g6}

    def attend(k, peak):
        u = 2 * k
        peak_b = scores(u + 1, score_b)
        weigh(u, score_a, peak)
        peak_a = scores(jnp.minimum(u + 2, 15), score_a)
        weigh(u + 1, score_b, peak_b)

        @pl.when(lax.rem(k, 2) == 1)
        def _():
            att_copy(k // 2).start()

        for when, event in events.items():
            pl.when(k == when)(event)
        return peak_a

    lax.fori_loop(0, 8, attend, scores(0, score_a))

    def row_pair(c):
        return -c, c + 1

    def project(t, c):
        parts = [
            wg[pl.ds(4 * wrap(y + r, N_Y), 4)].reshape(N_X * PAD, 2 * K_DEV)
            for r in row_pair(c)
        ]
        w = jnp.concatenate(parts, axis=0)
        rows = tile_rows(t)
        return nt(att[0, rows, :], w[:, :K_DEV]) + nt(att[1, rows, :], w[:, K_DEV:])

    routes = (zp, zm, zp, zm, zp, zm)

    def rs_copy(c, k):
        return copy(INDEX["rs00"] + 6 * c + k, snd.at[c, k], rcv.at[c, k], routes[k])

    def ship(c, k, value):
        snd[c, k] = value.astype(BF16)
        rs_copy(c, k).start()

    def landed(c, k):
        await_recv(INDEX["rs00"] + 6 * c + k, rcv.at[c, k])
        return rcv[c, k].astype(F32)

    def fi_copy(c):
        return copy(INDEX["fi0"] + c, hrecv.at[1, c], hrecv.at[2, c], partner)

    def phase1(c):
        for r in row_pair(c):
            yy = y + r
            await_recv(INDEX["bx0F"] + 3 * r, b_block(x + 2, yy))

        def one(n, carry):
            value = project(tile_at(n), c)

            @pl.when(n == 0)
            def _():
                ship(c, 0, value[:HALF])
                ship(c, 1, value[HALF:])

            @pl.when(n == 1)
            def _():
                ship(c, 2, value[HALF:])
                fin[0, c] = value[:HALF]

            @pl.when(n == 2)
            def _():
                ship(c, 3, value[:HALF])
                fin[1, c] = value[HALF:]

            @pl.when(n == 3)
            def _():
                fin[2, c] = value[:HALF]
                fin[3, c] = value[HALF:]

            return carry

        lax.fori_loop(0, 4, one, 0)

    def phase2(c):
        ship(c, 4, fin[0, c] + landed(c, 0))
        ship(c, 5, fin[1, c] + landed(c, 1))

    def phase3(c):
        top = fin[2, c] + landed(c, 4) + landed(c, 3)
        low_half = fin[3, c] + landed(c, 5) + landed(c, 2)
        hrecv[0, c] = jnp.where(core == 0, top, low_half).astype(BF16)
        hrecv[1, c] = jnp.where(core == 0, low_half, top).astype(BF16)
        fi_copy(c).start()

    def phase4(c):
        await_recv(INDEX["fi0"] + c, hrecv.at[2, c])
        for hf in range(2):
            r = nn(hrecv[0, c], sel[hf, core]) + nn(hrecv[2, c], sel[hf, 1 - core])
            res_rows[wrap(y + row_pair(c)[hf], N_Y)] = r.astype(BF16)

    def make_selection():
        shape = (CHUNK, CHUNK)

        def one(n, carry):
            hf, z = n // 2, lax.rem(n, 2)
            inner = ids(shape, 0) - hf * N_X * PAD
            block = sum((inner >= PAD * i).astype(jnp.int32) for i in (1, 2, 3))
            j = inner - PAD * block
            inside = (inner >= 0) & (inner < N_X * PAD) & (j < COLS)
            target = jnp.where(inside, COLS * (2 * block + z) + j, -1)
            sel[hf, z] = (ids(shape, 1) == target).astype(F32).astype(BF16)
            return carry

        lax.fori_loop(0, 4, one, 0)

    for n in range(4):
        att_ready(n)

    def step(i, carry):
        @pl.when(i == 1)
        def _():
            g7()

        @pl.when(i == 2)
        def _():
            g8()
            g9()

        @pl.when(i == 3)
        def _():
            g10()
            got("ay4")

        pl.when(i < 4)(lambda: phase1(i))
        pl.when(i == 0)(make_selection)
        pl.when((i >= 1) & (i < 5))(lambda: phase2(i - 1))
        pl.when((i >= 3) & (i < 7))(lambda: phase3(i - 3))
        pl.when(i >= 4)(lambda: phase4(i - 4))
        return carry

    lax.fori_loop(0, 8, step, 0)

    width = N_X * 2 * COLS
    for i in range(N_Y):
        out_ref[:, pl.ds(width * i, width)] = res_rows[i][:, :width]

    for name, (src, _, device) in messages.items():
        copy(INDEX[name], src, src, device).wait_send()

    def drain(c, carry):
        att_copy(c).wait_send()
        fi_copy(c).wait_send()
        for k in range(6):
            rs_copy(c, k).wait_send()
        return carry

    lax.fori_loop(0, 4, drain, 0)
    far.wait_send()

    @pl.when(zl != core)
    def _():
        near.wait_send()


def per_device(
    tree_queries, tree_keys, tree_values, cache_keys, cache_values, sinks, parents, tile_counts, out_weight
):
    vmem = pl.BlockSpec(memory_space=pltpu.VMEM)
    smem = pl.BlockSpec(memory_space=pltpu.SMEM)
    keys = CTX + TREE
    count = len(NAMES)
    out = pl.pallas_call(
        kernel,
        out_shape=jax.ShapeDtypeStruct((HALF, N_Y * N_X * 2 * COLS), BF16),
        in_specs=[vmem, vmem, vmem, vmem, vmem, smem, vmem, smem, vmem],
        out_specs=vmem,
        scratch_shapes=[
            pltpu.VMEM((PAD, K_DEV), BF16),
            pltpu.VMEM((N_Y * N_X, PAD, 2 * K_DEV), BF16),
            pltpu.VMEM((keys, 2 * HEAD_DIM), BF16),
            pltpu.VMEM((VROWS, keys), BF16),
            pltpu.VMEM((TREE, TREE), F32),
            pltpu.VMEM((2, BLOCK, BLOCK), BF16),
            pltpu.VMEM((2, TREE, K_DEV), BF16),
            pltpu.VMEM((4, 6, HALF, CHUNK), BF16),
            pltpu.VMEM((4, 6, HALF, CHUNK), BF16),
            pltpu.VMEM((4, 4, HALF, CHUNK), F32),
            pltpu.VMEM((3, 4, HALF, CHUNK), BF16),
            pltpu.VMEM((2, 2, CHUNK, CHUNK), BF16),
            pltpu.VMEM((N_Y, HALF, CHUNK), BF16),
            pltpu.VMEM((keys, 2 * TILE), F32),
            pltpu.VMEM((keys, 2 * TILE), F32),
            pltpu.SemaphoreType.DMA((count,)),
            pltpu.SemaphoreType.DMA((count,)),
            pltpu.SemaphoreType.DMA,
        ],
        compiler_params=pltpu.CompilerParams(collective_id=0, has_side_effects=True),
    )(
        tree_queries[0], tree_keys[0].T, tree_values[0].T, cache_keys[0].T, cache_values[0].T,
        sinks, parents, tile_counts, out_weight.T,
    )
    return out[None]


def solution(mesh):
    sizes = (N_Y, N_X, N_ZL, N_ZH, N_CORE)
    split = Mesh(mesh.devices.reshape(sizes), (*REQ, *TP))
    placed = (
        P(REQ, None, TP),
        P(REQ, None, TP),
        P(REQ, None, TP),
        P(REQ, None, TP),
        P(REQ, None, TP),
        P(TP),
        P(REQ, None),
        P(REQ),
        P(TP, REQ),
    )
    return jax.shard_map(
        per_device, mesh=split, in_specs=placed, out_specs=P(REQ, TP, None), check_vma=False
    )
```

```python
import jax
import jax.numpy as jnp
from jax import lax
from jax.experimental import pallas as pl
from jax.experimental.pallas import tpu as pltpu
from jax.sharding import Mesh
from jax.sharding import PartitionSpec as P

HEADS = 64
KV_HEADS = 8
HEAD_DIM = 64
TREE = 512
TILE = 128
CTX = 1024
N_Y, N_X, N_ZL, N_ZH, N_CORE = 8, 4, 2, 4, 2
COLS = 45
PAD = 48
CUT = 16
K_DEV = 512
CHUNK = 2 * N_X * PAD
HALF = TILE // 2
BLOCK = TREE // 2
VROWS = HEAD_DIM + 16
masked_score = -1e30
MESH = pl.DeviceIdType.MESH
REQ = ("y", "x", "zl")
TP = ("zh", "core")
F32 = jnp.float32
BF16 = jnp.bfloat16


def nt(a, b):
    return lax.dot_general(a, b, (((1,), (1,)), ((), ())), preferred_element_type=F32)


def nn(a, b):
    return jnp.dot(a, b, preferred_element_type=F32)


def ids(shape, dim):
    return lax.broadcasted_iota(jnp.int32, shape, dim)


ROW_OFFSETS = (0, 1, -1, 2, -2, 3, -3, 4)
NAMES = (
    ["s0", "s1"]
    + ["ax" + k for k in "PMF"]
    + ["ay%d" % r for r in range(-3, 5) if r]
    + ["by%d" % r for r in range(-3, 5) if r]
    + ["bx%d%s" % (r, k) for r in range(-3, 5) for k in "PMF"]
    + ["at%d" % t for t in range(4)]
    + ["rs%d%d" % (c, k) for c in range(4) for k in range(6)]
    + ["fi%d" % c for c in range(4)]
)
INDEX = {name: i for i, name in enumerate(NAMES)}


def kernel(
    q_ref, tk_ref, tv_ref, ck_ref, cv_ref, sink_ref, par_ref, cnt_ref, w_ref,
    out_ref,
    wt, wg, k2, vx, bias, reach, att, snd, rcv, fin, hrecv, sel, res_rows, score_a, score_b,
    send_sem, recv_sem, local_sem,
):
    y, x, zl = lax.axis_index("y"), lax.axis_index("x"), lax.axis_index("zl")
    zh, core = lax.axis_index("zh"), lax.axis_index("core")
    d = 1 - 2 * core

    def wrap(a, n):
        return lax.rem(a + n, n)

    xp, xm, xd = ({"x": wrap(x + s, N_X)} for s in (1, -1, d))
    yp, ym, yd = ({"y": wrap(y + s, N_Y)} for s in (1, -1, d))
    zp, zm = ({"zh": wrap(zh + s, N_ZH)} for s in (1, -1))
    partner = {"core": 1 - core}

    barrier = pltpu.get_barrier_semaphore()
    peers = [partner, xp, xm, yp, ym, zp, zm]
    peers += [{"zl": 1 - zl, "core": 0}, {"zl": 1 - zl, "core": 1}]
    for peer in peers:
        pl.semaphore_signal(barrier, inc=1, device_id=peer, device_id_type=MESH)

    block = w_ref[...].astype(F32)
    wt[...] = jnp.concatenate([block, jnp.zeros((PAD - COLS, K_DEV), F32)], axis=0).astype(BF16)
    pl.semaphore_wait(barrier, len(peers))

    def copy(i, src, dst, device):
        return pltpu.make_async_remote_copy(
            src_ref=src, dst_ref=dst, send_sem=send_sem.at[i], recv_sem=recv_sem.at[i],
            device_id=device, device_id_type=MESH,
        )

    def await_recv(i, dst):
        copy(i, dst, dst, partner).wait_recv()

    def slot(xx, yy):
        return 4 * wrap(yy, N_Y) + wrap(xx, N_X)

    own = slot(x, y)

    def lanes(k):
        return pl.ds(pl.multiple_of(k * K_DEV, K_DEV), K_DEV)

    mine = wg.at[own, :, lanes(core)]
    far = pltpu.make_async_remote_copy(
        src_ref=wt, dst_ref=mine, send_sem=send_sem.at[INDEX["s0"]],
        recv_sem=recv_sem.at[core], device_id={"zl": 1 - zl, "core": zl}, device_id_type=MESH,
    )
    far.start()
    near = pltpu.make_async_remote_copy(
        src_ref=wt, dst_ref=mine, send_sem=send_sem.at[INDEX["s1"]],
        recv_sem=recv_sem.at[core], device_id=partner, device_id_type=MESH,
    )
    here = pltpu.make_async_copy(wt, mine, local_sem)

    @pl.when(zl == core)
    def _():
        here.start()

    @pl.when(zl != core)
    def _():
        near.start()

    def a_block(xx, yy):
        return wg.at[slot(xx, yy), pl.ds(0, CUT), :]

    def a_row(yy):
        return wg.at[pl.ds(4 * wrap(yy, N_Y), 4), pl.ds(0, CUT), :]

    def b_block(xx, yy):
        return wg.at[slot(xx, yy), pl.ds(CUT, PAD - CUT), :]

    messages = {
        "axP": (a_block(x, y), a_block(x - 1, y), xp),
        "axM": (a_block(x, y), a_block(x + 1, y), xm),
        "axF": (a_block(x - d, y), a_block(x + 2, y), xd),
        "ay4": (a_row(y - 3 * d), a_row(y + 4), yd),
        "by4": (b_block(x, y - 3 * d), b_block(x, y + 4), yd),
    }
    for k in (1, 2, 3):
        messages["ay%d" % -k] = (a_row(y - k + 1), a_row(y - k), yp)
        messages["ay%d" % k] = (a_row(y + k - 1), a_row(y + k), ym)
        messages["by%d" % -k] = (b_block(x, y - k + 1), b_block(x, y - k), yp)
        messages["by%d" % k] = (b_block(x, y + k - 1), b_block(x, y + k), ym)
    for r in ROW_OFFSETS:
        messages["bx%dP" % r] = (b_block(x, y + r), b_block(x - 1, y + r), xp)
        messages["bx%dM" % r] = (b_block(x, y + r), b_block(x + 1, y + r), xm)
        messages["bx%dF" % r] = (b_block(x - d, y + r), b_block(x + 2, y + r), xd)

    def go(name):
        src, _, device = messages[name]
        copy(INDEX[name], src, src, device).start()

    def got(name):
        await_recv(INDEX[name], messages[name][1])

    def begin_gather():
        for k in range(2):
            part = wg.at[own, :, pl.ds(k * K_DEV, K_DEV)]
            waiting = pltpu.make_async_remote_copy(
                src_ref=part, dst_ref=part, send_sem=send_sem.at[0], recv_sem=recv_sem.at[k],
                device_id=partner, device_id_type=MESH,
            )

            @pl.when((zl != core) | (core != k))
            def _():
                waiting.wait_recv()

        @pl.when(zl == core)
        def _():
            here.wait()

        for name in ("axP", "axM", "by1", "by-1", "bx0P", "bx0M"):
            go(name)

    def row_b(r):
        got("by%d" % r)
        if abs(r) < 3:
            go("by%d" % (r + (1 if r > 0 else -1)))
        go("bx%dP" % r)
        go("bx%dM" % r)

    def last_hop(kind):
        go("%sy4" % kind)

    def relay(r):
        got("bx%dP" % r)
        got("bx%dM" % r)
        go("bx%dF" % r)

    def row_a(r):
        got("ay%d" % r)
        if abs(r) < 3:
            go("ay%d" % (r + (1 if r > 0 else -1)))

    def g1():
        got("axP")
        got("axM")
        go("axF")

    def g3():
        got("axF")
        go("ay1")
        go("ay-1")

    def g5():
        row_a(1)
        row_a(-1)

    def g6():
        row_b(3)
        row_b(-3)
        last_hop("b")
        relay(2)
        relay(-2)

    def g7():
        row_a(2)
        row_a(-2)

    def g8():
        got("by4")
        go("bx4P")
        go("bx4M")
        relay(3)
        relay(-3)

    def g9():
        row_a(3)
        row_a(-3)
        last_hop("a")

    def g10():
        relay(4)

    for source, at, length in ((ck_ref, 0, CTX), (tk_ref, CTX, TREE)):
        keys = source[...].astype(F32)
        k2[pl.ds(at, length), :] = jnp.concatenate([keys, keys], axis=0).T.astype(BF16)
    vx[pl.ds(0, HEAD_DIM), pl.ds(0, CTX)] = cv_ref[...]
    vx[pl.ds(0, HEAD_DIM), pl.ds(CTX, TREE)] = tv_ref[...]
    vx[pl.ds(HEAD_DIM, VROWS - HEAD_DIM), :] = jnp.ones((VROWS - HEAD_DIM, CTX + TREE), BF16)

    square = (BLOCK, BLOCK)

    def parent_of(j0, i0):
        return (ids(square, 0) + j0) == par_ref[:, pl.ds(i0, BLOCK)]

    for i in range(2):
        edge = parent_of(i * BLOCK, i * BLOCK) | (ids(square, 0) == ids(square, 1))
        reach[i] = edge.astype(F32).astype(BF16)

    begin_gather()

    def squaring(_, carry):
        twice = [nn(reach[i], reach[i]) for i in range(2)]
        for i in range(2):
            reach[i] = (twice[i] > 0.5).astype(F32).astype(BF16)
        return carry

    lax.fori_loop(0, 4, squaring, 0)
    g1()
    lax.fori_loop(0, 4, squaring, 0)
    across = nn(reach[0], parent_of(0, BLOCK).astype(F32).astype(BF16)).astype(BF16)
    across = nn(across, reach[1])

    def as_bias(seen):
        return jnp.where(seen.astype(F32) > 0.5, 0.0, masked_score)

    bias[pl.ds(0, BLOCK), pl.ds(0, BLOCK)] = as_bias(reach[0])
    bias[pl.ds(0, BLOCK), pl.ds(BLOCK, BLOCK)] = as_bias(across)
    bias[pl.ds(BLOCK, BLOCK), pl.ds(0, BLOCK)] = jnp.full(square, masked_score, F32)
    bias[pl.ds(BLOCK, BLOCK), pl.ds(BLOCK, BLOCK)] = as_bias(reach[1])

    low = ids((TILE, TILE), 1) < HEAD_DIM
    first = ids((1, 2 * TILE), 1) < TILE
    live_tiles = cnt_ref[0]
    opp, up_t, dn_t = wrap(zh + 2, N_ZH), wrap(zh + 1, N_ZH), wrap(zh - 1, N_ZH)

    def tile_at(n):
        shift = jnp.where(n == 0, 2, jnp.where(n == 1, 1, jnp.where(n == 2, 3, 0)))
        return lax.rem(zh + shift, N_ZH)

    def tile_rows(t):
        return pl.ds(pl.multiple_of(t * TILE, TILE), TILE)

    def columns_of(u):
        return pl.ds(pl.multiple_of(lax.rem(u, 4) * TILE, TILE), TILE)

    def sink_of(u):
        p = lax.rem(u, 4)
        return jnp.where(first, sink_ref[2 * p], sink_ref[2 * p + 1])

    def scores(u, store):
        rows = tile_rows(tile_at(u // 4))
        both = q_ref[rows, columns_of(u)].astype(F32) * (HEAD_DIM**-0.5)
        q2 = jnp.concatenate(
            [jnp.where(low, both, 0.0), jnp.where(low, 0.0, both)], axis=0
        ).astype(BF16)
        top = None
        for i in range((CTX + TREE) // BLOCK):
            s = nt(k2[pl.ds(i * BLOCK, BLOCK), :], q2)
            if i * BLOCK >= CTX:
                mask = bias[pl.ds(i * BLOCK - CTX, BLOCK), rows]
                s = s + jnp.concatenate([mask, mask], axis=1)
            store[pl.ds(i * BLOCK, BLOCK), :] = s
            part = s.reshape(BLOCK // 8, 8, 2 * TILE).max(0)
            top = part if top is None else jnp.maximum(top, part)
        return jnp.maximum(top.max(0, keepdims=True), sink_of(u))

    def weigh(u, store, peak):
        t = tile_at(u // 4)
        o = None
        for i in range((CTX + TREE) // BLOCK):
            keys = pl.ds(i * BLOCK, BLOCK)
            p = jnp.exp(store[keys, :] - peak).astype(BF16)
            part = nn(vx[:, keys], p)
            o = part if o is None else o + part
        den = o[HEAD_DIM : HEAD_DIM + 1] + jnp.exp(sink_of(u) - peak)
        res = o[:HEAD_DIM] / den
        res = jnp.concatenate([res[:, :TILE], res[:, TILE:]], axis=0).T
        res = jnp.where(t < live_tiles, res, 0.0)
        att[core, tile_rows(t), columns_of(u)] = res.astype(BF16)

    def att_copy(n):
        part = att.at[core, tile_rows(tile_at(n)), :]
        return copy(INDEX["at0"] + n, part, part, partner)

    def att_ready(n):
        await_recv(INDEX["at0"] + n, att.at[1 - core, tile_rows(tile_at(n)), :])

    def step_1():
        row_b(1)
        row_b(-1)

    def step_2():
        relay(0)

    def step_4():
        row_b(2)
        row_b(-2)
        relay(1)
        relay(-1)

    events = {0: step_1, 1: step_2, 2: g3, 4: step_4, 6: g5, 7: g6}

    def attend(k, peak):
        u = 2 * k
        peak_b = scores(u + 1, score_b)
        weigh(u, score_a, peak)
        peak_a = scores(jnp.minimum(u + 2, 15), score_a)
        weigh(u + 1, score_b, peak_b)

        @pl.when(lax.rem(k, 2) == 1)
        def _():
            att_copy(k // 2).start()

        for when, event in events.items():
            pl.when(k == when)(event)
        return peak_a

    lax.fori_loop(0, 8, attend, scores(0, score_a))

    def row_pair(c):
        return -c, c + 1

    def project(t, c):
        parts = [
            wg[pl.ds(4 * wrap(y + r, N_Y), 4)].reshape(N_X * PAD, 2 * K_DEV)
            for r in row_pair(c)
        ]
        w = jnp.concatenate(parts, axis=0)
        rows = tile_rows(t)
        return nt(att[0, rows, :], w[:, :K_DEV]) + nt(att[1, rows, :], w[:, K_DEV:])

    routes = (zp, zm, zp, zm, zp, zm)

    def rs_copy(c, k):
        return copy(INDEX["rs00"] + 6 * c + k, snd.at[c, k], rcv.at[c, k], routes[k])

    def ship(c, k, value):
        snd[c, k] = value.astype(BF16)
        rs_copy(c, k).start()

    def landed(c, k):
        await_recv(INDEX["rs00"] + 6 * c + k, rcv.at[c, k])
        return rcv[c, k].astype(F32)

    def fi_copy(c):
        return copy(INDEX["fi0"] + c, hrecv.at[1, c], hrecv.at[2, c], partner)

    def phase1(c):
        for r in row_pair(c):
            yy = y + r
            await_recv(INDEX["bx0F"] + 3 * r, b_block(x + 2, yy))

        def one(n, carry):
            value = project(tile_at(n), c)

            @pl.when(n == 0)
            def _():
                ship(c, 0, value[:HALF])
                ship(c, 1, value[HALF:])

            @pl.when(n == 1)
            def _():
                ship(c, 2, value[HALF:])
                fin[0, c] = value[:HALF]

            @pl.when(n == 2)
            def _():
                ship(c, 3, value[:HALF])
                fin[1, c] = value[HALF:]

            @pl.when(n == 3)
            def _():
                fin[2, c] = value[:HALF]
                fin[3, c] = value[HALF:]

            return carry

        lax.fori_loop(0, 4, one, 0)

    def phase2(c):
        ship(c, 4, fin[0, c] + landed(c, 0))
        ship(c, 5, fin[1, c] + landed(c, 1))

    def phase3(c):
        top = fin[2, c] + landed(c, 4) + landed(c, 3)
        low_half = fin[3, c] + landed(c, 5) + landed(c, 2)
        hrecv[0, c] = jnp.where(core == 0, top, low_half).astype(BF16)
        hrecv[1, c] = jnp.where(core == 0, low_half, top).astype(BF16)
        fi_copy(c).start()

    def phase4(c):
        await_recv(INDEX["fi0"] + c, hrecv.at[2, c])
        for hf in range(2):
            r = nn(hrecv[0, c], sel[hf, core]) + nn(hrecv[2, c], sel[hf, 1 - core])
            res_rows[wrap(y + row_pair(c)[hf], N_Y)] = r.astype(BF16)

    def make_selection():
        shape = (CHUNK, CHUNK)

        def one(n, carry):
            hf, z = n // 2, lax.rem(n, 2)
            inner = ids(shape, 0) - hf * N_X * PAD
            block = sum((inner >= PAD * i).astype(jnp.int32) for i in (1, 2, 3))
            j = inner - PAD * block
            inside = (inner >= 0) & (inner < N_X * PAD) & (j < COLS)
            target = jnp.where(inside, COLS * (2 * block + z) + j, -1)
            sel[hf, z] = (ids(shape, 1) == target).astype(F32).astype(BF16)
            return carry

        lax.fori_loop(0, 4, one, 0)

    for n in range(4):
        att_ready(n)

    def step(i, carry):
        @pl.when(i == 1)
        def _():
            g7()

        @pl.when(i == 2)
        def _():
            g8()
            g9()

        @pl.when(i == 3)
        def _():
            g10()
            got("ay4")

        phase1(i)
        pl.when(i == 0)(make_selection)
        pl.when(i >= 1)(lambda: phase2(i - 1))
        return carry

    lax.fori_loop(0, 4, step, 0)
    phase3(0)
    phase3(1)
    phase4(0)
    phase2(3)
    phase4(1)
    phase3(2)
    phase4(2)
    phase3(3)
    phase4(3)

    width = N_X * 2 * COLS
    for i in range(N_Y):
        out_ref[:, pl.ds(width * i, width)] = res_rows[i][:, :width]

    for name, (src, _, device) in messages.items():
        copy(INDEX[name], src, src, device).wait_send()

    def drain(c, carry):
        att_copy(c).wait_send()
        fi_copy(c).wait_send()
        for k in range(6):
            rs_copy(c, k).wait_send()
        return carry

    lax.fori_loop(0, 4, drain, 0)
    far.wait_send()

    @pl.when(zl != core)
    def _():
        near.wait_send()


def per_device(
    tree_queries, tree_keys, tree_values, cache_keys, cache_values, sinks, parents, tile_counts, out_weight
):
    vmem = pl.BlockSpec(memory_space=pltpu.VMEM)
    smem = pl.BlockSpec(memory_space=pltpu.SMEM)
    keys = CTX + TREE
    count = len(NAMES)
    out = pl.pallas_call(
        kernel,
        out_shape=jax.ShapeDtypeStruct((HALF, N_Y * N_X * 2 * COLS), BF16),
        in_specs=[vmem, vmem, vmem, vmem, vmem, smem, vmem, smem, vmem],
        out_specs=vmem,
        scratch_shapes=[
            pltpu.VMEM((PAD, K_DEV), BF16),
            pltpu.VMEM((N_Y * N_X, PAD, 2 * K_DEV), BF16),
            pltpu.VMEM((keys, 2 * HEAD_DIM), BF16),
            pltpu.VMEM((VROWS, keys), BF16),
            pltpu.VMEM((TREE, TREE), F32),
            pltpu.VMEM((2, BLOCK, BLOCK), BF16),
            pltpu.VMEM((2, TREE, K_DEV), BF16),
            pltpu.VMEM((4, 6, HALF, CHUNK), BF16),
            pltpu.VMEM((4, 6, HALF, CHUNK), BF16),
            pltpu.VMEM((4, 4, HALF, CHUNK), F32),
            pltpu.VMEM((3, 4, HALF, CHUNK), BF16),
            pltpu.VMEM((2, 2, CHUNK, CHUNK), BF16),
            pltpu.VMEM((N_Y, HALF, CHUNK), BF16),
            pltpu.VMEM((keys, 2 * TILE), F32),
            pltpu.VMEM((keys, 2 * TILE), F32),
            pltpu.SemaphoreType.DMA((count,)),
            pltpu.SemaphoreType.DMA((count,)),
            pltpu.SemaphoreType.DMA,
        ],
        compiler_params=pltpu.CompilerParams(collective_id=0, has_side_effects=True),
    )(
        tree_queries[0], tree_keys[0].T, tree_values[0].T, cache_keys[0].T, cache_values[0].T,
        sinks, parents, tile_counts, out_weight.T,
    )
    return out[None]


def solution(mesh):
    sizes = (N_Y, N_X, N_ZL, N_ZH, N_CORE)
    split = Mesh(mesh.devices.reshape(sizes), (*REQ, *TP))
    placed = (
        P(REQ, None, TP),
        P(REQ, None, TP),
        P(REQ, None, TP),
        P(REQ, None, TP),
        P(REQ, None, TP),
        P(TP),
        P(REQ, None),
        P(REQ),
        P(TP, REQ),
    )
    return jax.shard_map(
        per_device, mesh=split, in_specs=placed, out_specs=P(REQ, TP, None), check_vma=False
    )
```
